32 devices in a mesh: dp: 8 (over z, y), mp: 4 (over x, core).
Axes of the slice: x: 2, y: 2, z: 4, core: 2. Of those that a mesh axis runs over, the one named last changes fastest.
Arguments:
- x_in: bfloat16 [8, 1024, 1024], P('dp'), may hold values from -6 to 6
- segments: int32 [8, 1024], P('dp'), may hold values from 0 to 3, as said below
- levels: int32 [8, 1024], P('dp'), may hold values from 0 to 9, as said below
- lengths: int32 [8, 4], P('dp'), may hold values from 1 to 680, as said below
- labels: int32 [8, 4], P('dp'), may hold values from 0 to 999
- targets: int32 [8, 1024], P('dp'), may hold values from 0 to 4095
- owners: int32 [7], replicated, may hold values from 0 to 7, as said below
- step: int32 [1], replicated, may hold values from 1 to 20
- master: float32 [8, 4, 3145728], P('dp', 'mp'), may hold values from -4 to 4, as said below
- first: float32 [8, 4, 3145728], P('dp', 'mp'), may hold values from -6.67572e-06 to 6.67572e-06
- second: float32 [8, 4, 3145728], P('dp', 'mp'), may hold values from 8.0183814e-13 to 3.2073526e-12
Outputs:
- loss: float32 [], replicated
- grad_norm: float32 [], replicated
- act_rms: float32 [3], replicated
- master_out: float32 [8, 4, 3145728], P('dp', 'mp')
- first_out: float32 [8, 4, 3145728], P('dp', 'mp')
- second_out: float32 [8, 4, 3145728], P('dp', 'mp')
The draws below stay inside these ranges and needn't reach their ends.
Inputs may be any that keep to these rules, and one draw needn't show every extreme that they name: The images of a row in order; the first of each row has 680 tokens; every length is one of 1, 5, 14, 30, 55, 91, 155, 255, 424, 680, and a row's lengths sum to at most 1024. `segments`: image i covers its lengths' positions in order after images 0 to i - 1; positions after a row's last image carry 4 - 1. `levels`: for a position at place p of its image, the number of the counts 1, 5, 14, 30, 55, 91, 155, 255, 424, 680 that are at most p, capped at 10 - 1 (also past the last image). In the order Wqkv, Wo, Wup, Wdown, Wada, Whead, Wcls: Wup and Wada have the same owner, all other owners are distinct and differ from it. `master`: entries of each stored matrix have a spread of about its fan-in to the minus one half (Wo eight times, Whead twice, Wcls about one).
All inputs are finite; a program needn't handle non-finite values.
Results may differ from the reference program's by a relative error of at most 0.0058.
Values may be sent and summed in bfloat16 or wider, within the bound.
A program may use at most 384 MiB of HBM per device.

```python
import math
import jax
import jax.numpy as jnp
import numpy as np
from jax import lax

D = 1024
HEADS = 16
HEAD_DIM = 64
FF = 4096
VOCAB = 4096
CLASSES = 1000
LEVELS = 10
ITEMS = 4
ROW_LEN = 1024
N_ROWS = 8
PARAMS = 26189824
CAP = 3145728
N_DP = 8
N_MP = 4


PLAN = (1, 5, 14, 30, 55, 91, 155, 255, 424, 680)


def ragged(key):
    base = jax.random.fold_in(key, 7)
    table = jnp.array(PLAN, jnp.int32)
    second_len = table[jax.random.randint(jax.random.fold_in(base, 1), (N_ROWS, 1), 0, 8)]
    tail_len = table[jax.random.randint(jax.random.fold_in(base, 2), (N_ROWS, ITEMS - 2), 0, 4)]
    first_len = jnp.full((N_ROWS, 1), 680, jnp.int32)
    return jnp.concatenate([first_len, second_len, tail_len], 1)


def placement_of(key):
    lengths = ragged(key)
    ends = jnp.cumsum(lengths, 1)
    positions = jnp.arange(ROW_LEN, dtype=jnp.int32)
    segment = jnp.sum((positions[None, :, None] >= ends[:, None, :]).astype(jnp.int32), -1)
    segment = jnp.minimum(segment, ITEMS - 1)
    starts = ends - lengths
    begin = jnp.take_along_axis(starts, segment, axis=1)
    within = positions[None, :] - begin
    table = jnp.array(PLAN, jnp.int32)
    level = jnp.sum((within[:, :, None] >= table[None, None, :]).astype(jnp.int32), -1)
    level = jnp.minimum(level, LEVELS - 1)
    return (lengths, segment.astype(jnp.int32), level.astype(jnp.int32))


def draw_lengths(key, part):
    return placement_of(key)[0]


def draw_segments(key, part):
    return placement_of(key)[1]


def draw_levels(key, part):
    return placement_of(key)[2]


def owner_list(key):
    order = jax.random.permutation(jax.random.fold_in(key, 11), N_DP).astype(jnp.int32)
    return jnp.stack([order[1], order[2], order[0], order[3], order[0], order[4], order[5]]).astype(jnp.int32)


def draw_owners(key, part):
    return owner_list(key)


def draw_master(key, part):
    owners = owner_list(key)
    sizes = [3 * D * D // N_MP, D * D // N_MP, D * FF // N_MP, FF * D // N_MP, 8 * D * D // N_MP, D * VOCAB // N_MP, CLASSES * D // N_MP]
    offsets = [0, 0, 0, 0, D * FF // N_MP, 0, 0]
    spreads = [D ** (-0.5), 8.0 * D ** (-0.5), D ** (-0.5), FF ** (-0.5), D ** (-0.5), 2.0 * D ** (-0.5), 1.0]
    column = jnp.arange(CAP, dtype=jnp.int32)
    devices = jnp.arange(N_DP, dtype=jnp.int32)
    scale = jnp.full((N_DP, CAP), D ** (-0.5), jnp.float32)
    for matrix_id in range(7):
        inside = (devices[:, None] == owners[matrix_id]) & (column[None, :] >= offsets[matrix_id]) & (column[None, :] < offsets[matrix_id] + sizes[matrix_id])
        scale = jnp.where(inside, jnp.float32(spreads[matrix_id]), scale)
    noise = jax.random.truncated_normal(jax.random.fold_in(key, 13), -4.0, 4.0, (N_DP, N_MP, CAP), jnp.float32)
    return noise * scale[:, None, :]


def with_ends(values, key, low, high):
    extent = values.shape
    spot = [jax.random.randint(jax.random.fold_in(key, axis), (), 0, extent[axis]) for axis in range(len(extent))]
    values = values.at[tuple(spot)].set(low)
    longest = extent.index(max(extent))
    spot[longest] = (spot[longest] + 1) % extent[longest]
    return values.at[tuple(spot)].set(high)


def shard_levels(rng, shape, pieces, least, high):
    factor_of, own = 1.0, jax.random.fold_in(rng, 6)
    for position, shards_of in pieces:
        steps = jnp.exp(jax.random.uniform(jax.random.fold_in(own, position), (shards_of,), jnp.float32, least / len(pieces), high / len(pieces)))
        factor_of = factor_of * jnp.repeat(steps, shape[position] // shards_of).reshape([-1 if axis == position else 1 for axis in range(len(shape))])
    return factor_of


def cumulative_ranks(number_of, lean):
    loads = [(1 << 20) // math.isqrt(standing ** lean) + 1 for standing in range(1, number_of + 1)]
    deviation = 1 + sum(loads) // (1 << 30)
    return np.cumsum(np.array([max(1, weight // deviation) for weight in loads]))


def ranked(key, dims, amount, skew):
    grid = cumulative_ranks(amount, skew)
    pick = jax.random.randint(jax.random.fold_in(key, 1), dims, 0, int(grid[amount - 1]))
    grade = jnp.searchsorted(jnp.asarray(grid, jnp.int32), pick, side="right")
    return jax.random.permutation(jax.random.fold_in(key, 2), amount)[grade].astype(jnp.int32)


def centred(own_key, shape, deviation, most, cuts=(), kind=jnp.bfloat16):
    loudness = shard_levels(own_key, shape, cuts, -0.22, 0.18) if cuts else 1.0
    values = jax.random.normal(own_key, shape, jnp.float32) * deviation * loudness
    return jnp.minimum(jnp.maximum(values, -most), most).astype(kind)


def setup_inputs(seed: int = 0) -> dict:
    key_of = jax.random.split(jax.random.key(seed), 12)
    return {
        "x_in": centred(key_of[0], (N_ROWS, ROW_LEN, D), 1.0, 6.0, ((0, 8),)),
        "segments": draw_segments(jax.random.fold_in(key_of[11], 71), 0),
        "levels": draw_levels(jax.random.fold_in(key_of[11], 71), 0),
        "lengths": draw_lengths(jax.random.fold_in(key_of[11], 71), 0),
        "labels": with_ends(jax.random.randint(key_of[4], (N_ROWS, ITEMS), 0, CLASSES), jax.random.fold_in(key_of[4], 1), 0, CLASSES - 1).astype(jnp.int32),
        "targets": with_ends(ranked(key_of[5], (N_ROWS, ROW_LEN), VOCAB, 2), jax.random.fold_in(key_of[5], 3), 0, VOCAB - 1).astype(jnp.int32),
        "owners": draw_owners(jax.random.fold_in(key_of[11], 71), 0),
        "step": jax.random.randint(key_of[7], (1,), 1, 21).astype(jnp.int32),
        "master": draw_master(jax.random.fold_in(key_of[11], 71), 0),
        "first": centred(key_of[9], (N_DP, N_MP, CAP), (0.0022 / PARAMS ** 0.5), 6.67572021484375e-06, ((0, 8), (1, 4)), jnp.float32),
        "second": jnp.clip(jnp.exp(math.log(3.207352569298272e-12) - 1.3862944 * jax.random.uniform(key_of[10], (N_DP, N_MP, CAP), jnp.float32) ** shard_levels(key_of[10], (N_DP, N_MP, CAP), ((0, 8), (1, 4)), -0.2, 0.2)), 8.01838142324568e-13, 3.207352569298272e-12),
    }


BETA_ONE = 0.9
BETA_TWO = 0.95
ADAM_EPS = 1e-08
LEARN_RATE = 0.03
WEIGHT_DECAY = 0.05
CLIP_AT = 0.02
NORM_EPS = 1e-06
HIGH = lax.Precision.HIGHEST

@jax.custom_vjp
def low(v):
    return lax.optimization_barrier(v.astype(jnp.bfloat16)).astype(jnp.float32)

@jax.custom_vjp
def low_back(v):
    return v

def low_keep(v):
    return (low(v), None)

def low_pass(kept, grad):
    return (grad,)

def back_keep(v):
    return (v, None)

def back_low(kept, grad):
    return (low(grad),)
low.defvjp(low_keep, low_pass)
low_back.defvjp(back_keep, back_low)

def layer_norm(stream):
    centre = stream - lax.optimization_barrier(jnp.mean(stream, -1, keepdims=True))
    return centre * lax.rsqrt(lax.optimization_barrier(jnp.mean(centre * centre, -1, keepdims=True)) + NORM_EPS)

def matrix_layout():
    sizes = [3 * D * D // N_MP, D * D // N_MP, D * FF // N_MP, FF * D // N_MP, 8 * D * D // N_MP, D * VOCAB // N_MP, CLASSES * D // N_MP]
    shapes = [(D, 3, D // N_MP), (D // N_MP, D), (D, FF // N_MP), (FF // N_MP, D), (D // N_MP, 8 * D), (D, VOCAB // N_MP), (CLASSES, D // N_MP)]
    offsets = [0, 0, 0, 0, D * FF // N_MP, 0, 0]
    split_axes = [2, 0, 1, 0, 0, 1, 1]
    return (sizes, shapes, offsets, split_axes)

def unpack(buffer, owners):
    sizes, shapes, offsets, split_axes = matrix_layout()
    result = []
    for matrix_id in range(7):
        slot = lax.dynamic_index_in_dim(buffer, owners[matrix_id], 0, keepdims=False)
        shards = [slot[shard_id, offsets[matrix_id]:offsets[matrix_id] + sizes[matrix_id]].reshape(shapes[matrix_id]) for shard_id in range(N_MP)]
        result.append(jnp.concatenate(shards, split_axes[matrix_id]))
    return result

def pack(buffer, owners, fulls):
    sizes, shapes, offsets, split_axes = matrix_layout()
    for matrix_id in range(7):
        shards = jnp.split(fulls[matrix_id], N_MP, axis=split_axes[matrix_id])
        slot = lax.dynamic_index_in_dim(buffer, owners[matrix_id], 0, keepdims=False)
        for shard_id in range(N_MP):
            slot = slot.at[shard_id, offsets[matrix_id]:offsets[matrix_id] + sizes[matrix_id]].set(shards[shard_id].reshape(-1))
        buffer = lax.dynamic_update_index_in_dim(buffer, slot, owners[matrix_id], 0)
    return buffer

def row_terms(weights, stream, segment, level, lengths, label, target):
    w_qkv, w_proj, w_up, w_down, w_ada, w_head, w_class = weights
    positions = jnp.arange(ROW_LEN, dtype=jnp.int32)
    valid = (positions < jnp.cumsum(lengths)[-1]).astype(jnp.float32)
    cond = w_class[label]
    modulation = low_back(jnp.dot(low(jax.nn.silu(cond)), w_ada, precision=HIGH))
    per_token = modulation[segment]
    gate_one, scale_one, shift_one, gate_two, scale_two, shift_two, head_scale, head_shift = jnp.split(per_token, 8, axis=-1)
    mixed_in = low(layer_norm(stream) * (1.0 + scale_one) + shift_one)
    projected = jnp.einsum('ld,dkh->lkh', mixed_in, w_qkv, precision=HIGH).reshape(ROW_LEN, 3, HEADS, HEAD_DIM)
    queries = low(low_back(projected[:, 0]))
    keys_all = low(low_back(projected[:, 1]))
    values_all = low(low_back(projected[:, 2]))
    allowed = (segment[:, None] == segment[None, :]) & (level[None, :] <= level[:, None]) & (valid[None, :] > 0) | (positions[:, None] == positions[None, :])
    scores = low_back(jnp.einsum('qhd,khd->hqk', queries, keys_all, precision=HIGH) * HEAD_DIM ** (-0.5))
    scores = jnp.where(allowed[None], scores, -1e+30)
    probs = jax.nn.softmax(scores, axis=-1)
    context = low(low_back(jnp.einsum('hqk,khd->qhd', low(probs), values_all, precision=HIGH).reshape(ROW_LEN, D)))
    attended = low_back(jnp.dot(context, w_proj, precision=HIGH))
    middle = stream + gate_one * attended
    up_in = low(layer_norm(middle) * (1.0 + scale_two) + shift_two)
    hidden_pre = low_back(jnp.dot(up_in, w_up, precision=HIGH))
    activated = low(jax.nn.gelu(hidden_pre, approximate=True))
    branch = low_back(jnp.dot(activated, w_down, precision=HIGH))
    final = middle + gate_two * branch
    head_in = low(layer_norm(final) * (1.0 + head_scale) + head_shift)
    logits = low_back(jnp.dot(head_in, w_head, precision=HIGH))
    log_total = jax.nn.logsumexp(logits, axis=-1)
    picked = jnp.take_along_axis(logits, target[:, None], axis=-1)[:, 0]
    loss_sum = jnp.sum((log_total - picked) * valid)
    column = valid[:, None]
    return (loss_sum, jnp.sum(final * final * column), jnp.sum((gate_one * attended) ** 2 * column), jnp.sum((gate_two * branch) ** 2 * column))

def reference(x_in, segments, levels, lengths, labels, targets, owners, step, master, first, second):
    owners = owners.astype(jnp.int32)
    fulls = unpack(master, owners)
    weights = [full.astype(jnp.bfloat16).astype(jnp.float32) for full in fulls]
    count = jnp.sum(lengths).astype(jnp.float32)
    stream = x_in.astype(jnp.float32)

    def loss_of(weights):

        def row_step(carry, row):
            terms = row_terms(weights, *row)
            return (tuple((left + right for left, right in zip(carry, terms))), None)
        zero = jnp.zeros((), jnp.float32)
        totals, _ = lax.scan(jax.checkpoint(row_step), (zero, zero, zero, zero), (stream, segments, levels, lengths, labels, targets))
        return (totals[0] / count, totals)
    loss, pullback, totals = jax.vjp(loss_of, weights, has_aux=True)
    grads = pullback(jnp.ones_like(loss))[0]
    squares = sum((jnp.sum(grad * grad) for grad in grads))
    grad_norm = jnp.sqrt(squares)
    factor = jnp.minimum(1.0, CLIP_AT / (grad_norm + 1e-06))
    count_step = step[0].astype(jnp.float32)
    fix_one = 1.0 - BETA_ONE ** count_step
    fix_two = 1.0 - BETA_TWO ** count_step
    moments_one = unpack(first, owners)
    moments_two = unpack(second, owners)
    new_masters, new_ones, new_twos = ([], [], [])
    for matrix_id in range(7):
        grad_part = grads[matrix_id] * factor
        moment_one = BETA_ONE * moments_one[matrix_id] + (1.0 - BETA_ONE) * grad_part
        moment_two = BETA_TWO * moments_two[matrix_id] + (1.0 - BETA_TWO) * grad_part * grad_part
        updated = fulls[matrix_id] * (1.0 - LEARN_RATE * WEIGHT_DECAY) - LEARN_RATE * (moment_one / fix_one) / (jnp.sqrt(moment_two / fix_two) + ADAM_EPS)
        new_masters.append(updated)
        new_ones.append(moment_one)
        new_twos.append(moment_two)
    act_rms = jnp.sqrt(jnp.stack([totals[1], totals[2], totals[3]]) / (count * D))
    return (loss, grad_norm, act_rms, pack(master, owners, new_masters), pack(first, owners, new_ones), pack(second, owners, new_twos))
```

```python
from functools import partial

import jax
import jax.numpy as jnp
from jax import lax
from jax.sharding import PartitionSpec as P

D = 1024
HEADS = 16
HEAD_DIM = 64
FF = 4096
VOCAB = 4096
CLASSES = 1000
ITEMS = 4
ROW_LEN = 1024


BETA_ONE = 0.9
BETA_TWO = 0.95
ADAM_EPS = 1e-08
LEARN_RATE = 0.03
WEIGHT_DECAY = 0.05
CLIP_AT = 0.02
NORM_EPS = 1e-06
HIGH = lax.Precision.HIGHEST
BF = jnp.bfloat16
F32 = jnp.float32


def ring_of(count):
    return list(range(0, count, 2)) + list(range(count - 1, 0, -2))


def joined(value, axis, join):
    pieces = jax.tree.map(lambda part: lax.all_gather(part, axis), value)
    count = lax.axis_size(axis)
    total = jax.tree.map(lambda part: part[0], pieces)
    for place in range(1, count):
        total = join(total, jax.tree.map(lambda part: part[place], pieces))
    return total


def layer_norm(stream):
    centre = stream - jnp.mean(stream, -1, keepdims=True)
    inverse = lax.rsqrt(jnp.mean(centre * centre, -1, keepdims=True) + NORM_EPS)
    return (centre * inverse, inverse)


def norm_back(normed, inverse, upstream):
    return inverse * (
        upstream
        - jnp.mean(upstream, -1, keepdims=True)
        - normed * jnp.mean(upstream * normed, -1, keepdims=True)
    )


def contract_rows(left, right):
    return lax.dot_general(
        left, right, (((0,), (0,)), ((), ())), preferred_element_type=jnp.float32
    )


def contract_last(left, right):
    return lax.dot_general(
        left, right, (((1,), (1,)), ((), ())), preferred_element_type=jnp.float32
    )


def masked_scores(queries, keys_all, allowed):
    scores = jnp.einsum(
        "rqhd,rkhd->rhqk", queries, keys_all, preferred_element_type=jnp.float32
    ) * HEAD_DIM ** (-0.5)
    return jnp.where(allowed[:, None], scores, -1e30)


def combine_parts(one, two):
    larger = jnp.maximum(one[0], two[0])
    return (
        larger,
        one[1] * jnp.exp(one[0] - larger) + two[1] * jnp.exp(two[0] - larger),
        one[2] + two[2],
    )


def gather_ring(piece):
    count = lax.axis_size("dp")
    mine = lax.axis_index("dp")
    order = ring_of(count)
    place_table = jnp.array([order.index(d) for d in range(count)], jnp.int32)
    ring_table = jnp.array(order, jnp.int32)
    place = place_table[mine]
    right = [(order[i], order[(i + 1) % count]) for i in range(count)]
    left = [(b, a) for a, b in right]
    whole = jnp.zeros((piece.shape[0], count) + piece.shape[1:], piece.dtype)

    def put(whole, value, source, lower):
        return lax.dynamic_update_slice(
            whole, value[:, None], (0, source, lower, 0)
        )

    whole = put(whole, piece, mine, 0)
    half = piece.shape[1] // 2
    going, coming = piece, piece
    for step in range(1, count // 2 + 1):
        last = step == count // 2
        if last:
            going, coming = going[:, :half], coming[:, half:]
        going = lax.ppermute(going, "dp", right)
        coming = lax.ppermute(coming, "dp", left)
        whole = put(whole, going, ring_table[(place - step) % count], 0)
        whole = put(whole, coming, ring_table[(place + step) % count], half if last else 0)
    return whole


def reduce_pairs(parts):
    count = lax.axis_size("dp")
    mine = lax.axis_index("dp")
    half = count // 2
    k, _, b, d = parts.shape
    parity = mine % 2
    tall = mine // 2
    split = parts.reshape(k, half, 2, b, d)
    away = lax.dynamic_index_in_dim(split, 1 - parity, 2, keepdims=False).astype(BF)
    keep = lax.dynamic_index_in_dim(split, parity, 2, keepdims=False)
    got = lax.ppermute(away, "dp", [(s, s ^ 1) for s in range(count)])
    pair = keep + got.astype(F32)
    total = lax.dynamic_index_in_dim(pair, tall, 1, keepdims=False)
    for shift in range(1, half):
        out = lax.dynamic_index_in_dim(pair, (tall + shift) % half, 1, keepdims=False)
        move = [(s, ((s // 2 + shift) % half) * 2 + s % 2) for s in range(count)]
        total = total + lax.ppermute(out.astype(BF), "dp", move).astype(F32)
    return total


def per_device(
    x_in, segments, levels, lengths, labels, targets, owners, step, master, first, second
):
    ways = lax.axis_size("mp")
    count_dp = lax.axis_size("dp")
    mine = lax.axis_index("dp")
    flat_master = master.reshape(-1)
    flat_first = first.reshape(-1)
    flat_second = second.reshape(-1)
    rows = x_in.shape[0]
    tokens = rows * ROW_LEN
    share_rows = tokens // ways
    local_heads = HEADS // ways
    local_width = D // ways
    slot = D * FF // ways
    slot_rows = slot // D
    block = local_width // count_dp
    row_counts = [3 * local_width, local_width, slot_rows, slot_rows, slot_rows]
    matrix_of = [0, 1, 2, 3, 5]

    facts = lax.all_gather(jnp.concatenate([labels, lengths], -1), "dp", axis=0, tiled=True)
    all_labels = facts[:, :ITEMS].reshape(-1)
    count = jnp.sum(facts[:, ITEMS:]).astype(F32)

    low_slot = flat_master[:slot].astype(BF).reshape(-1, count_dp, block, D)
    shares = lax.all_to_all(low_slot.transpose(1, 0, 2, 3), "dp", 0, 0, tiled=True)
    pieces = [
        lax.dynamic_index_in_dim(shares, owners[m], 0, keepdims=False)[: r // (block * count_dp)]
        for m, r in zip(matrix_of, row_counts)
    ]
    early = gather_ring(jnp.concatenate(pieces[:2], 0))
    late = gather_ring(jnp.concatenate(pieces[2:], 0))
    k_qkv = pieces[0].shape[0]
    k_slot = pieces[2].shape[0]
    w_qkv = early[:k_qkv].reshape(D, 3, local_width)
    w_proj = early[k_qkv:].reshape(local_width, D)
    w_up = late[:k_slot].reshape(D, FF // ways)
    w_down = late[k_slot : 2 * k_slot].reshape(FF // ways, D)
    w_head = late[2 * k_slot :].reshape(D, VOCAB // ways)

    def own(values):
        return lax.dynamic_slice_in_dim(values, lax.axis_index("mp") * share_rows, share_rows, 0)

    def spread(share):
        return lax.all_gather(share, "mp", axis=0, tiled=True)

    def reduce_heads(term):
        return lax.psum_scatter(term, "mp", scatter_dimension=0, tiled=True)

    positions = jnp.arange(ROW_LEN, dtype=jnp.int32)
    ends = jnp.cumsum(lengths, -1)
    valid = (positions[None, :] < ends[:, -1:]).astype(F32)
    flat_valid = valid.reshape(-1)
    item_ids = (jnp.arange(rows, dtype=jnp.int32)[:, None] * ITEMS + segments).reshape(-1)
    flat_hits = (item_ids[:, None] == jnp.arange(rows * ITEMS, dtype=jnp.int32)[None, :]).astype(
        F32
    )
    share_ids = own(item_ids)
    share_hits = own(flat_hits)

    def item_sums(values, hits):
        return jnp.einsum("ln,ld->nd", hits, values, precision=HIGH).reshape(rows, ITEMS, D)

    class_size = CLASSES * local_width
    owns_class = owners[6] == mine
    owns_ada = owners[4] == mine
    class_rows = flat_master[:class_size].astype(BF).reshape(CLASSES, local_width)
    picks = (all_labels[:, None] == jnp.arange(CLASSES, dtype=jnp.int32)[None, :]).astype(BF)
    cond_low = jnp.dot(picks, class_rows, preferred_element_type=F32)
    cond = lax.psum(jnp.where(owns_class, cond_low, 0.0), "dp")
    silu_out, silu_back = jax.vjp(jax.nn.silu, cond)
    cond_act = silu_out.astype(BF)
    w_ada = flat_master[slot : 3 * slot].astype(BF).reshape(local_width, 8 * D)
    mod_part = jnp.dot(cond_act, w_ada, preferred_element_type=F32)
    mod_all = lax.all_to_all(mod_part.reshape(count_dp, rows * ITEMS, 8 * D), "dp", 0, 0, tiled=True)
    modulation = lax.psum(lax.dynamic_index_in_dim(mod_all, owners[4], 0, keepdims=False), "mp")

    def per_token(place, ids):
        table = modulation[:, place * D : (place + 1) * D]
        result = jnp.broadcast_to(table[0][None], (ids.shape[0], D))
        for item in range(1, rows * ITEMS):
            result = jnp.where((ids == item)[:, None], table[item][None], result)
        return result

    scale_one, shift_one = per_token(1, item_ids), per_token(2, item_ids)
    gate_one_own, gate_two_own = per_token(0, share_ids), per_token(3, share_ids)
    scale_two_own, shift_two_own = per_token(4, share_ids), per_token(5, share_ids)
    head_scale_own, head_shift_own = per_token(6, share_ids), per_token(7, share_ids)

    stream = x_in.astype(F32).reshape(tokens, D)
    normed_one, inverse_one = layer_norm(stream)
    mixed_in = (normed_one * (1.0 + scale_one) + shift_one).astype(BF)
    projected = jnp.einsum(
        "nd,dkh->nkh", mixed_in, w_qkv, preferred_element_type=jnp.float32
    ).astype(BF)
    projected = projected.reshape(rows, ROW_LEN, 3, local_heads, HEAD_DIM)
    queries = projected[:, :, 0]
    keys_all = projected[:, :, 1]
    values_all = projected[:, :, 2]
    allowed = (segments[:, :, None] == segments[:, None, :]) & (
        levels[:, None, :] <= levels[:, :, None]
    ) & (valid[:, None, :] > 0) | (positions[:, None] == positions[None, :])[None]
    scores = masked_scores(queries, keys_all, allowed)
    highest = jnp.max(scores, -1, keepdims=True)
    raised = jnp.exp(scores - highest)
    summed = jnp.sum(raised, -1, keepdims=True)
    probs = raised / summed
    log_norm = highest + jnp.log(summed)
    context = (
        jnp.einsum(
            "rhqk,rkhd->rqhd",
            probs.astype(BF),
            values_all,
            preferred_element_type=jnp.float32,
        )
        .astype(BF)
        .reshape(tokens, local_width)
    )
    attended = reduce_heads(jnp.dot(context, w_proj, preferred_element_type=jnp.float32))
    middle = own(stream) + gate_one_own * attended
    normed_two, inverse_two = layer_norm(middle)
    up_in = spread((normed_two * (1.0 + scale_two_own) + shift_two_own).astype(BF))
    hidden_pre = jnp.dot(up_in, w_up, preferred_element_type=jnp.float32)
    gelu_out, gelu_back = jax.vjp(partial(jax.nn.gelu, approximate=True), hidden_pre)
    activated = gelu_out.astype(BF)
    branch = reduce_heads(jnp.dot(activated, w_down, preferred_element_type=jnp.float32))
    final = middle + gate_two_own * branch
    normed_head, inverse_head = layer_norm(final)
    head_in = spread((normed_head * (1.0 + head_scale_own) + head_shift_own).astype(BF))
    logits = jnp.dot(head_in, w_head, preferred_element_type=jnp.float32)
    vocab_ids = (
        jnp.arange(logits.shape[1], dtype=jnp.int32) + lax.axis_index("mp") * logits.shape[1]
    )
    target_hits = vocab_ids[None, :] == targets.reshape(-1)[:, None]
    local_top = jnp.max(logits, -1)
    local_sum = jnp.sum(jnp.exp(logits - local_top[:, None]), -1)
    local_pick = jnp.sum(jnp.where(target_hits, logits, 0.0), -1)
    global_top, global_sum, picked = joined((local_top, local_sum, local_pick), "mp", combine_parts)
    log_total = global_top + jnp.log(global_sum)
    column = own(flat_valid)[:, None]
    attn_part = gate_one_own * attended
    mlp_part = gate_two_own * branch
    square_terms = (
        jnp.sum(final * final * column),
        jnp.sum(attn_part * attn_part * column),
        jnp.sum(mlp_part * mlp_part * column),
    )
    first_mp = (lax.axis_index("mp") == 0).astype(F32)
    loss_term = jnp.sum((log_total - picked) * flat_valid) * first_mp
    soft = jnp.exp(logits - log_total[:, None])
    logit_grad = ((soft - target_hits.astype(F32)) * (flat_valid / count)[:, None]).astype(BF)

    def by_block(grad):
        return grad.reshape(-1, count_dp, block, D)

    grad_head = contract_rows(head_in, logit_grad)
    share_head = reduce_pairs(by_block(grad_head))
    head_in_grad = reduce_heads(contract_last(logit_grad, w_head))
    grad_head_scale = head_in_grad * normed_head
    final_grad = norm_back(normed_head, inverse_head, head_in_grad * (1.0 + head_scale_own))
    branch_grad = spread((final_grad * gate_two_own).astype(BF))
    grad_gate_two = final_grad * branch
    grad_down = contract_rows(activated, branch_grad)
    hidden_grad = gelu_back(contract_last(branch_grad, w_down))[0].astype(BF)
    grad_up = contract_rows(up_in, hidden_grad)
    share_ff = reduce_pairs(jnp.concatenate([by_block(grad_down), by_block(grad_up)], 0))
    up_in_grad = reduce_heads(contract_last(hidden_grad, w_up))
    grad_scale_two = up_in_grad * normed_two
    middle_grad = final_grad + norm_back(
        normed_two, inverse_two, up_in_grad * (1.0 + scale_two_own)
    )
    attended_grad = spread((middle_grad * gate_one_own).astype(BF))
    grad_gate_one = middle_grad * attended
    grad_proj = contract_rows(context, attended_grad)
    context_grad = (
        contract_last(attended_grad, w_proj)
        .astype(BF)
        .reshape(rows, ROW_LEN, local_heads, HEAD_DIM)
    )
    probs_again = jnp.exp(masked_scores(queries, keys_all, allowed) - log_norm)
    probs_grad = jnp.einsum(
        "rqhd,rkhd->rhqk", context_grad, values_all, preferred_element_type=jnp.float32
    )
    values_grad = jnp.einsum(
        "rhqk,rqhd->rkhd",
        probs_again.astype(BF),
        context_grad,
        preferred_element_type=jnp.float32,
    )
    scores_grad = (
        probs_again * (probs_grad - jnp.sum(probs_again * probs_grad, -1, keepdims=True))
    ).astype(BF)
    queries_grad = jnp.einsum(
        "rhqk,rkhd->rqhd", scores_grad, keys_all, preferred_element_type=jnp.float32
    ) * HEAD_DIM ** (-0.5)
    keys_grad = jnp.einsum(
        "rhqk,rqhd->rkhd", scores_grad, queries, preferred_element_type=jnp.float32
    ) * HEAD_DIM ** (-0.5)
    projected_grad = (
        jnp.stack([queries_grad, keys_grad, values_grad], axis=2)
        .astype(BF)
        .reshape(tokens, 3, local_width)
    )
    grad_qkv = jnp.einsum(
        "nd,nkh->dkh", mixed_in, projected_grad, preferred_element_type=jnp.float32
    )
    share_attn = reduce_pairs(
        jnp.concatenate([by_block(grad_qkv.reshape(-1, D)), by_block(grad_proj)], 0)
    )
    mixed_grad_part = jnp.einsum(
        "nkh,dkh->nd", projected_grad, w_qkv, preferred_element_type=jnp.float32
    )
    local_items = (
        item_sums(grad_gate_one, share_hits),
        item_sums(mixed_grad_part * normed_one, flat_hits),
        item_sums(mixed_grad_part, flat_hits),
        item_sums(grad_gate_two, share_hits),
        item_sums(grad_scale_two, share_hits),
        item_sums(up_in_grad, share_hits),
        item_sums(grad_head_scale, share_hits),
        item_sums(head_in_grad, share_hits),
    )
    items = lax.psum(jnp.concatenate(local_items, axis=-1), "mp")
    mod_grad = lax.all_gather(
        items.reshape(rows * ITEMS, 8 * D).astype(BF), "dp", axis=0, tiled=True
    )
    grad_ada = contract_rows(cond_act, mod_grad)
    cond_part = contract_last(mod_grad, w_ada)
    cond_grad = silu_back(lax.psum(jnp.where(owns_ada, cond_part, 0.0), "dp"))[0]
    class_hits = (all_labels[:, None] == jnp.arange(CLASSES, dtype=jnp.int32)[None, :]).astype(F32)
    grad_class = jnp.einsum("nc,nd->cd", class_hits, cond_grad, precision=HIGH)

    squares = (
        jnp.sum(share_head * share_head)
        + jnp.sum(share_ff * share_ff)
        + jnp.sum(share_attn * share_attn)
        + jnp.where(owns_ada, jnp.sum(grad_ada * grad_ada), 0.0)
        + jnp.where(owns_class, jnp.sum(grad_class * grad_class), 0.0)
    )
    norm_terms = lax.psum((squares, loss_term) + square_terms, ("dp", "mp"))
    grad_norm = jnp.sqrt(norm_terms[0])
    loss = norm_terms[1] / count
    factor = jnp.minimum(1.0, CLIP_AT / (grad_norm + 1e-06))

    chunk = jnp.zeros((count_dp, k_slot, block, D), BF)
    summed_shares = [
        share_attn[:k_qkv],
        share_attn[k_qkv:],
        share_ff[k_slot:],
        share_ff[:k_slot],
        share_head,
    ]
    for m, part in zip(matrix_of, summed_shares):
        chunk = lax.dynamic_update_slice(chunk, part.astype(BF)[None], (owners[m], 0, 0, 0))
    got = lax.all_to_all(chunk, "dp", 0, 0, tiled=True)
    slot_grad = got.transpose(1, 0, 2, 3).reshape(-1).astype(F32)
    class_flat = jnp.pad(grad_class.reshape(-1), (0, slot - class_size))
    slot_grad = jnp.where(owns_class, class_flat, slot_grad)
    sizes = [r * D for r in row_counts] + [class_size]
    slot_size = jnp.zeros((), jnp.int32)
    for m, size in zip(matrix_of + [6], sizes):
        slot_size = jnp.where(owners[m] == mine, size, slot_size)
    ada_size = jnp.where(owns_ada, 2 * slot, 0)

    count_step = step[0].astype(F32)
    fix_one = 1.0 - BETA_ONE**count_step
    fix_two = 1.0 - BETA_TWO**count_step

    def adam(grad, size, lower, upper):
        w, m, v = flat_master[lower:upper], flat_first[lower:upper], flat_second[lower:upper]
        grad = grad * factor
        moment_one = BETA_ONE * m + (1.0 - BETA_ONE) * grad
        moment_two = BETA_TWO * v + (1.0 - BETA_TWO) * grad * grad
        updated = w * (1.0 - LEARN_RATE * WEIGHT_DECAY) - LEARN_RATE * (moment_one / fix_one) / (
            jnp.sqrt(moment_two / fix_two) + ADAM_EPS
        )
        inside = jnp.arange(upper - lower, dtype=jnp.int32) < size
        return (
            jnp.where(inside, updated, w),
            jnp.where(inside, moment_one, m),
            jnp.where(inside, moment_two, v),
        )

    low_part = adam(slot_grad, slot_size, 0, slot)
    high_part = adam(grad_ada.reshape(-1), ada_size, slot, 3 * slot)
    outs = [
        jnp.concatenate([a, b]).reshape(master.shape) for a, b in zip(low_part, high_part)
    ]
    act_rms = jnp.sqrt(jnp.stack(norm_terms[2:]) / (count * D))
    return (loss, grad_norm, act_rms, *outs)


def solution(mesh):
    placed = (
        P("dp", None, None),
        P("dp", None),
        P("dp", None),
        P("dp", None),
        P("dp", None),
        P("dp", None),
        P(),
        P(),
        P("dp", "mp", None),
        P("dp", "mp", None),
        P("dp", "mp", None),
    )
    return jax.shard_map(
        per_device,
        mesh=mesh,
        in_specs=placed,
        out_specs=(P(), P(), P(), P("dp", "mp", None), P("dp", "mp", None), P("dp", "mp", None)),
        check_vma=False,
    )
```

```python
from functools import partial

import jax
import jax.numpy as jnp
from jax import lax
from jax.experimental import pallas as pl
from jax.experimental.pallas import tpu as pltpu
from jax.sharding import PartitionSpec as P

D = 1024
HEADS = 16
HEAD_DIM = 64
FF = 4096
VOCAB = 4096
CLASSES = 1000
ITEMS = 4
ROW_LEN = 1024


BETA_ONE = 0.9
BETA_TWO = 0.95
ADAM_EPS = 1e-08
LEARN_RATE = 0.03
WEIGHT_DECAY = 0.05
CLIP_AT = 0.02
NORM_EPS = 1e-06
HIGH = lax.Precision.HIGHEST
BF = jnp.bfloat16
F32 = jnp.float32


def ring_of(count):
    return list(range(0, count, 2)) + list(range(count - 1, 0, -2))


def layer_norm(stream):
    centre = stream - jnp.mean(stream, -1, keepdims=True)
    inverse = lax.rsqrt(jnp.mean(centre * centre, -1, keepdims=True) + NORM_EPS)
    return (centre * inverse, inverse)


def norm_back(normed, inverse, upstream):
    return inverse * (
        upstream
        - jnp.mean(upstream, -1, keepdims=True)
        - normed * jnp.mean(upstream * normed, -1, keepdims=True)
    )


def contract_rows(left, right):
    return lax.dot_general(
        left, right, (((0,), (0,)), ((), ())), preferred_element_type=jnp.float32
    )


def contract_last(left, right):
    return lax.dot_general(
        left, right, (((1,), (1,)), ((), ())), preferred_element_type=jnp.float32
    )


def masked_scores(queries, keys_all, allowed):
    scores = jnp.einsum(
        "rqhd,rkhd->rhqk", queries, keys_all, preferred_element_type=jnp.float32
    ) * HEAD_DIM ** (-0.5)
    return jnp.where(allowed[:, None], scores, -1e30)


LANES = 128
MESH = pl.DeviceIdType.MESH


def gather_small(value, axes, ident):
    sizes = [lax.axis_size(axis) for axis in axes]
    count = 1
    for size in sizes:
        count *= size

    def kernel(value_ref, out_ref, send_sem, recv_sem):
        mine = jnp.int32(0)
        for axis, size in zip(axes, sizes):
            mine = mine * size + lax.axis_index(axis)

        def peer(shift):
            place = lax.rem(mine + shift, count)
            where = {}
            for axis, size in zip(reversed(axes), reversed(sizes)):
                where[axis] = lax.rem(place, size)
                place = place // size
            return where

        def copy_to(shift):
            return pltpu.make_async_remote_copy(
                src_ref=value_ref,
                dst_ref=out_ref.at[mine],
                send_sem=send_sem.at[shift],
                recv_sem=recv_sem.at[shift],
                device_id=peer(shift),
                device_id_type=MESH,
            )

        barrier = pltpu.get_barrier_semaphore()

        @pl.loop(1, count)
        def _(shift):
            pl.semaphore_signal(barrier, inc=1, device_id=peer(shift), device_id_type=MESH)

        pl.semaphore_wait(barrier, count - 1)

        @pl.loop(1, count)
        def _(shift):
            copy_to(shift).start()

        out_ref[mine] = value_ref[...]

        @pl.loop(1, count)
        def _(shift):
            copy_to(shift).wait()

    return pl.pallas_call(
        kernel,
        out_shape=jax.ShapeDtypeStruct((count,) + value.shape, value.dtype),
        in_specs=[pl.BlockSpec(memory_space=pltpu.VMEM)],
        out_specs=pl.BlockSpec(memory_space=pltpu.VMEM),
        scratch_shapes=[
            pltpu.SemaphoreType.DMA((count,)),
            pltpu.SemaphoreType.DMA((count,)),
        ],
        compiler_params=pltpu.CompilerParams(collective_id=ident, has_side_effects=True),
        name=f"gather_small_{ident}",
    )(value)


def unflatten(flat_view, first_row, rows, width, step):
    wide = width // LANES
    view_step = step * wide
    assert first_row % view_step == 0 and rows % step == 0
    base = first_row // view_step

    def kernel(in_ref, out_ref):
        for place in range(wide):
            out_ref[:, place * LANES : (place + 1) * LANES] = in_ref[
                pl.ds(place, step, stride=wide), :
            ].astype(BF)

    return pl.pallas_call(
        kernel,
        out_shape=jax.ShapeDtypeStruct((rows, width), BF),
        grid=(rows // step,),
        in_specs=[pl.BlockSpec((view_step, LANES), lambda i: (i + base, 0))],
        out_specs=pl.BlockSpec((step, width), lambda i: (i, 0)),
        cost_estimate=pl.CostEstimate(
            flops=rows * width, bytes_accessed=6 * rows * width, transcendentals=0
        ),
        name=f"unflatten_{width}",
    )(flat_view)


def adam_kernel(
    steps, group, ada_rows, reals, whole, slot_ref, class_ref, act_ref, mod_ref,
    w_ref, m_ref, v_ref, w_out, m_out, v_out, grad_ref,
):
    place = pl.program_id(0)
    wide = D // LANES
    ada_wide = 8 * D // LANES

    @pl.when(place < steps)
    def _():
        use_class = jnp.logical_and(whole[1] > 0, place == 0)
        grad = jnp.where(use_class, class_ref[...], slot_ref[...].astype(F32))
        for j in range(wide):
            grad_ref[pl.ds(j, group, stride=wide), :] = grad[:, j * LANES : (j + 1) * LANES]

    @pl.when(place >= steps)
    def _():
        grad = jnp.dot(act_ref[...], mod_ref[...], preferred_element_type=F32)
        for j in range(ada_wide):
            grad_ref[pl.ds(j, ada_rows, stride=ada_wide), :] = grad[:, j * LANES : (j + 1) * LANES]

    limit = jnp.where(place < steps, (whole[0] - place * group) * wide, whole[2])
    inside = lax.broadcasted_iota(jnp.int32, grad_ref.shape, 0) < limit
    w, m, v = w_ref[...], m_ref[...], v_ref[...]
    grad = grad_ref[...] * reals[0]
    moment_one = BETA_ONE * m + (1.0 - BETA_ONE) * grad
    moment_two = BETA_TWO * v + (1.0 - BETA_TWO) * grad * grad
    updated = w * (1.0 - LEARN_RATE * WEIGHT_DECAY) - LEARN_RATE * (moment_one / reals[1]) / (
        jnp.sqrt(moment_two / reals[2]) + ADAM_EPS
    )
    w_out[...] = jnp.where(inside, updated, w)
    m_out[...] = jnp.where(inside, moment_one, m)
    v_out[...] = jnp.where(inside, moment_two, v)


def adam_step(reals, whole, slot_grad, class_grad, act, mod_grad, w, m, v):
    group = class_grad.shape[0]
    steps = slot_grad.shape[0] // group
    view = group * D // LANES
    ada_rows = group * D // (8 * D)
    items = mod_grad.shape[0]
    big = pl.BlockSpec((view, LANES), lambda i: (i, 0))
    smem = pl.BlockSpec(memory_space=pltpu.SMEM)
    shape = jax.ShapeDtypeStruct(w.shape, F32)
    return pl.pallas_call(
        partial(adam_kernel, steps, group, ada_rows),
        out_shape=(shape, shape, shape),
        grid=(3 * steps,),
        in_specs=[
            smem,
            smem,
            pl.BlockSpec((group, D), lambda i: (jnp.minimum(i, steps - 1), 0)),
            pl.BlockSpec((group, D), lambda i: (0, 0)),
            pl.BlockSpec((ada_rows, items), lambda i: (jnp.maximum(i - steps, 0), 0)),
            pl.BlockSpec((items, 8 * D), lambda i: (0, 0)),
            big,
            big,
            big,
        ],
        out_specs=(big, big, big),
        scratch_shapes=[pltpu.VMEM((view, LANES), F32)],
        name="adam_step",
    )(reals, whole, slot_grad, class_grad, act, mod_grad, w, m, v)


def gather_ring(piece):
    count = lax.axis_size("dp")
    mine = lax.axis_index("dp")
    order = ring_of(count)
    place_table = jnp.array([order.index(d) for d in range(count)], jnp.int32)
    ring_table = jnp.array(order, jnp.int32)
    place = place_table[mine]
    right = [(order[i], order[(i + 1) % count]) for i in range(count)]
    left = [(b, a) for a, b in right]
    whole = jnp.zeros((piece.shape[0], count) + piece.shape[1:], piece.dtype)

    def put(whole, value, source, lower):
        return lax.dynamic_update_slice(
            whole, value[:, None], (0, source, lower, 0)
        )

    whole = put(whole, piece, mine, 0)
    half = piece.shape[1] // 2
    going, coming = piece, piece
    for step in range(1, count // 2 + 1):
        last = step == count // 2
        if last:
            going, coming = going[:, :half], coming[:, half:]
        going = lax.ppermute(going, "dp", right)
        coming = lax.ppermute(coming, "dp", left)
        whole = put(whole, going, ring_table[(place - step) % count], 0)
        whole = put(whole, coming, ring_table[(place + step) % count], half if last else 0)
    return whole


def reduce_pairs(parts):
    count = lax.axis_size("dp")
    mine = lax.axis_index("dp")
    half = count // 2
    k, _, b, d = parts.shape
    parity = mine % 2
    tall = mine // 2
    split = parts.reshape(k, half, 2, b, d)
    away = lax.dynamic_index_in_dim(split, 1 - parity, 2, keepdims=False)
    keep = lax.dynamic_index_in_dim(split, parity, 2, keepdims=False)
    got = lax.ppermute(away, "dp", [(s, s ^ 1) for s in range(count)])

    def pair(shift):
        place = (tall + shift) % half
        one = lax.dynamic_index_in_dim(keep, place, 1, keepdims=False)
        two = lax.dynamic_index_in_dim(got, place, 1, keepdims=False)
        return one.astype(F32) + two.astype(F32)

    total = pair(0)
    for shift in range(1, half):
        move = [(s, ((s // 2 + shift) % half) * 2 + s % 2) for s in range(count)]
        total = total + lax.ppermute(pair(shift).astype(BF), "dp", move).astype(F32)
    return total


def core_mates():
    return [(s, s ^ 1) for s in range(lax.axis_size("mp"))]


def chip_moves(shift):
    chips = lax.axis_size("mp") // 2
    return [
        (s, ((s // 2 + shift) % chips) * 2 + s % 2) for s in range(lax.axis_size("mp"))
    ]


def reduce_heads(product, left):
    chips = lax.axis_size("mp") // 2
    half = left.shape[0] // 2
    share = half // chips
    away = product(left[half:]).astype(BF)
    got = lax.ppermute(away, "mp", core_mates())
    pair = product(left[:half]) + got.astype(F32)
    total = pair[:share]
    for shift in range(1, chips):
        out = pair[shift * share : (shift + 1) * share].astype(BF)
        total = total + lax.ppermute(out, "mp", chip_moves(shift)).astype(F32)
    return total


def spread(share):
    chips = lax.axis_size("mp") // 2
    half = jnp.concatenate(
        [share]
        + [lax.ppermute(share, "mp", chip_moves(chips - shift)) for shift in range(1, chips)]
    )
    return jnp.concatenate([half, lax.ppermute(half, "mp", core_mates())])


def per_device(
    x_in, segments, levels, lengths, labels, targets, owners, step, master, first, second
):
    ways = lax.axis_size("mp")
    count_dp = lax.axis_size("dp")
    mine = lax.axis_index("dp")
    master_view = master.reshape(-1, LANES)
    first_view = first.reshape(-1, LANES)
    second_view = second.reshape(-1, LANES)
    rows = x_in.shape[0]
    tokens = rows * ROW_LEN
    share_rows = tokens // ways
    local_heads = HEADS // ways
    local_width = D // ways
    slot = D * FF // ways
    slot_rows = slot // D
    block = local_width // count_dp
    row_counts = [3 * local_width, local_width, slot_rows, slot_rows, slot_rows]
    matrix_of = [0, 1, 2, 3, 5]

    assert rows == 1

    facts = jnp.concatenate([labels, lengths], -1).reshape(1, -1)
    facts = jnp.pad(facts, ((0, 7), (0, LANES - facts.shape[1])))
    facts = gather_small(facts, ("dp",), 1)[:, 0, : 2 * ITEMS]
    all_labels = facts[:, :ITEMS].reshape(-1)
    count = jnp.sum(facts[:, ITEMS:]).astype(F32)

    low_slot = unflatten(master_view, 0, slot_rows, D, local_width)
    split_slot = low_slot.reshape(-1, count_dp, block, D)
    shares = lax.all_to_all(split_slot.transpose(1, 0, 2, 3), "dp", 0, 0, tiled=True)
    pieces = [
        lax.dynamic_index_in_dim(shares, owners[m], 0, keepdims=False)[: r // (block * count_dp)]
        for m, r in zip(matrix_of, row_counts)
    ]
    early = gather_ring(jnp.concatenate(pieces[:2], 0))
    late = gather_ring(jnp.concatenate(pieces[2:], 0))
    k_qkv = pieces[0].shape[0]
    k_slot = pieces[2].shape[0]
    w_qkv = early[:k_qkv].reshape(D, 3, local_width)
    w_proj = early[k_qkv:].reshape(local_width, D)
    w_up = late[:k_slot].reshape(D, FF // ways)
    w_down = late[k_slot : 2 * k_slot].reshape(FF // ways, D)
    w_head = late[2 * k_slot :].reshape(D, VOCAB // ways)

    chips = ways // 2
    mine_mp = lax.axis_index("mp")

    def moved(values, places, axis):
        return jnp.concatenate(
            [
                lax.dynamic_slice_in_dim(values, place * share_rows, share_rows, axis)
                for place in places
            ],
            axis,
        )

    def localize(values, axis=0):
        places = [
            ((mine_mp // 2 + shift) % chips) * 2 + (mine_mp % 2 + other) % 2
            for other in range(2)
            for shift in range(chips)
        ]
        return moved(values, places, axis)

    def globalize(values, axis=0):
        places = [
            ((mine_mp + place) % 2) * chips + (place // 2 - mine_mp // 2 + chips) % chips
            for place in range(ways)
        ]
        return moved(values, places, axis)

    def own(values):
        return values[:share_rows]

    positions = localize(jnp.arange(ROW_LEN, dtype=jnp.int32))
    x_local = localize(x_in.reshape(tokens, D))
    segments, levels, targets = [
        localize(table.reshape(tokens)).reshape(table.shape) for table in (segments, levels, targets)
    ]
    ends = jnp.cumsum(lengths, -1)
    valid = (positions[None, :] < ends[:, -1:]).astype(F32)
    flat_valid = valid.reshape(-1)
    item_ids = (jnp.arange(rows, dtype=jnp.int32)[:, None] * ITEMS + segments).reshape(-1)
    flat_hits = (item_ids[:, None] == jnp.arange(rows * ITEMS, dtype=jnp.int32)[None, :]).astype(
        F32
    )
    share_ids = own(item_ids)
    share_hits = own(flat_hits)

    def item_sums(values, hits):
        return jnp.einsum("ln,ld->nd", hits, values, precision=HIGH).reshape(rows, ITEMS, D)

    owns_class = owners[6] == mine
    owns_ada = owners[4] == mine
    row_ids = jnp.arange(local_width, dtype=jnp.int32)
    picks = (all_labels[:, None] // ways == row_ids[None, :]).astype(BF)
    found = jnp.dot(picks, low_slot[:local_width], preferred_element_type=F32)
    cond_low = jnp.zeros((found.shape[0], local_width), F32)
    for part in range(ways):
        cond_low = jnp.where(
            (all_labels % ways == part)[:, None],
            found[:, part * local_width : (part + 1) * local_width],
            cond_low,
        )
    cond = jnp.sum(gather_small(jnp.where(owns_class, cond_low, 0.0), ("dp",), 2), 0)
    silu_out, silu_back = jax.vjp(jax.nn.silu, cond)
    cond_act = silu_out.astype(BF)
    w_ada = unflatten(master_view, slot // LANES, local_width, 8 * D, local_width // 8)
    mod_part = jnp.dot(cond_act, w_ada, preferred_element_type=F32)
    mod_all = lax.all_to_all(mod_part.reshape(count_dp, rows * ITEMS, 8 * D), "dp", 0, 0, tiled=True)
    mod_mine = lax.dynamic_index_in_dim(mod_all, owners[4], 0, keepdims=False)
    modulation = jnp.sum(gather_small(mod_mine.reshape(-1, D), ("mp",), 3), 0)
    modulation = modulation.reshape(rows * ITEMS, 8 * D)

    def per_token(place, ids):
        table = modulation[:, place * D : (place + 1) * D]
        result = jnp.broadcast_to(table[0][None], (ids.shape[0], D))
        for item in range(1, rows * ITEMS):
            result = jnp.where((ids == item)[:, None], table[item][None], result)
        return result

    scale_one, shift_one = per_token(1, item_ids), per_token(2, item_ids)
    gate_one_own, gate_two_own = per_token(0, share_ids), per_token(3, share_ids)
    scale_two_own, shift_two_own = per_token(4, share_ids), per_token(5, share_ids)
    head_scale_own, head_shift_own = per_token(6, share_ids), per_token(7, share_ids)

    stream = x_local.astype(F32)
    normed_one, inverse_one = layer_norm(stream)
    mixed_in = (normed_one * (1.0 + scale_one) + shift_one).astype(BF)
    projected = jnp.einsum(
        "nd,dkh->nkh", mixed_in, w_qkv, preferred_element_type=jnp.float32
    ).astype(BF)
    projected = projected.reshape(rows, ROW_LEN, 3, local_heads, HEAD_DIM)
    queries = projected[:, :, 0]
    keys_all = projected[:, :, 1]
    values_all = projected[:, :, 2]
    allowed = (segments[:, :, None] == segments[:, None, :]) & (
        levels[:, None, :] <= levels[:, :, None]
    ) & (valid[:, None, :] > 0) | (positions[:, None] == positions[None, :])[None]
    scores = masked_scores(queries, keys_all, allowed)
    highest = jnp.max(scores, -1, keepdims=True)
    raised = jnp.exp(scores - highest)
    summed = jnp.sum(raised, -1, keepdims=True)
    probs = raised / summed
    log_norm = highest + jnp.log(summed)
    context = (
        jnp.einsum(
            "rhqk,rkhd->rqhd",
            probs.astype(BF),
            values_all,
            preferred_element_type=jnp.float32,
        )
        .astype(BF)
        .reshape(tokens, local_width)
    )
    attended = reduce_heads(
        lambda part: jnp.dot(part, w_proj, preferred_element_type=jnp.float32), context
    )
    middle = own(stream) + gate_one_own * attended
    normed_two, inverse_two = layer_norm(middle)
    up_in = spread((normed_two * (1.0 + scale_two_own) + shift_two_own).astype(BF))
    hidden_pre = jnp.dot(up_in, w_up, preferred_element_type=jnp.float32)
    gelu_out, gelu_back = jax.vjp(partial(jax.nn.gelu, approximate=True), hidden_pre)
    activated = gelu_out.astype(BF)
    branch = reduce_heads(
        lambda part: jnp.dot(part, w_down, preferred_element_type=jnp.float32), activated
    )
    final = middle + gate_two_own * branch
    normed_head, inverse_head = layer_norm(final)
    head_in = spread((normed_head * (1.0 + head_scale_own) + head_shift_own).astype(BF))
    logits = jnp.dot(head_in, w_head, preferred_element_type=jnp.float32)
    vocab_ids = (
        jnp.arange(logits.shape[1], dtype=jnp.int32) + lax.axis_index("mp") * logits.shape[1]
    )
    target_hits = vocab_ids[None, :] == targets.reshape(-1)[:, None]
    local_top = jnp.max(logits, -1)
    local_sum = jnp.sum(jnp.exp(logits - local_top[:, None]), -1)
    local_pick = jnp.sum(jnp.where(target_hits, logits, 0.0), -1)
    stats = [globalize(values) for values in (local_top, local_sum, local_pick)]
    stats = gather_small(jnp.concatenate(stats).reshape(-1, LANES), ("mp",), 4)
    stats = localize(stats.reshape(ways, 3, tokens), 2)
    global_top = jnp.max(stats[:, 0], 0)
    global_sum = jnp.sum(stats[:, 1] * jnp.exp(stats[:, 0] - global_top[None]), 0)
    picked = jnp.sum(stats[:, 2], 0)
    log_total = global_top + jnp.log(global_sum)
    column = own(flat_valid)[:, None]
    attn_part = gate_one_own * attended
    mlp_part = gate_two_own * branch
    square_terms = (
        jnp.sum(final * final * column),
        jnp.sum(attn_part * attn_part * column),
        jnp.sum(mlp_part * mlp_part * column),
    )
    first_mp = (lax.axis_index("mp") == 0).astype(F32)
    loss_term = jnp.sum((log_total - picked) * flat_valid) * first_mp
    soft = jnp.exp(logits - log_total[:, None])
    logit_grad = ((soft - target_hits.astype(F32)) * (flat_valid / count)[:, None]).astype(BF)

    def by_block(grad):
        return grad.astype(BF).reshape(-1, count_dp, block, D)

    grad_head = contract_rows(head_in, logit_grad)
    share_head = reduce_pairs(by_block(grad_head))
    head_in_grad = reduce_heads(lambda part: contract_last(part, w_head), logit_grad)
    grad_head_scale = head_in_grad * normed_head
    final_grad = norm_back(normed_head, inverse_head, head_in_grad * (1.0 + head_scale_own))
    branch_grad = spread((final_grad * gate_two_own).astype(BF))
    grad_gate_two = final_grad * branch
    grad_down = contract_rows(activated, branch_grad)
    hidden_grad = gelu_back(contract_last(branch_grad, w_down))[0].astype(BF)
    grad_up = contract_rows(up_in, hidden_grad)
    share_down = reduce_pairs(by_block(grad_down))
    share_up = reduce_pairs(by_block(grad_up))
    up_in_grad = reduce_heads(lambda part: contract_last(part, w_up), hidden_grad)
    grad_scale_two = up_in_grad * normed_two
    middle_grad = final_grad + norm_back(
        normed_two, inverse_two, up_in_grad * (1.0 + scale_two_own)
    )
    attended_grad = spread((middle_grad * gate_one_own).astype(BF))
    grad_gate_one = middle_grad * attended
    grad_proj = contract_rows(context, attended_grad)
    context_grad = (
        contract_last(attended_grad, w_proj)
        .astype(BF)
        .reshape(rows, ROW_LEN, local_heads, HEAD_DIM)
    )
    probs_again = jnp.exp(masked_scores(queries, keys_all, allowed) - log_norm)
    probs_grad = jnp.einsum(
        "rqhd,rkhd->rhqk", context_grad, values_all, preferred_element_type=jnp.float32
    )
    values_grad = jnp.einsum(
        "rhqk,rqhd->rkhd",
        probs_again.astype(BF),
        context_grad,
        preferred_element_type=jnp.float32,
    )
    scores_grad = (
        probs_again * (probs_grad - jnp.sum(probs_again * probs_grad, -1, keepdims=True))
    ).astype(BF)
    queries_grad = jnp.einsum(
        "rhqk,rkhd->rqhd", scores_grad, keys_all, preferred_element_type=jnp.float32
    ) * HEAD_DIM ** (-0.5)
    keys_grad = jnp.einsum(
        "rhqk,rqhd->rkhd", scores_grad, queries, preferred_element_type=jnp.float32
    ) * HEAD_DIM ** (-0.5)
    projected_grad = (
        jnp.stack([queries_grad, keys_grad, values_grad], axis=2)
        .astype(BF)
        .reshape(tokens, 3, local_width)
    )
    grad_qkv = jnp.einsum(
        "nd,nkh->dkh", mixed_in, projected_grad, preferred_element_type=jnp.float32
    )
    share_attn = reduce_pairs(
        jnp.concatenate([by_block(grad_qkv.reshape(-1, D)), by_block(grad_proj)], 0)
    )
    mixed_grad_part = jnp.einsum(
        "nkh,dkh->nd", projected_grad, w_qkv, preferred_element_type=jnp.float32
    )
    local_items = (
        item_sums(grad_gate_one, share_hits),
        item_sums(mixed_grad_part * normed_one, flat_hits),
        item_sums(mixed_grad_part, flat_hits),
        item_sums(grad_gate_two, share_hits),
        item_sums(grad_scale_two, share_hits),
        item_sums(up_in_grad, share_hits),
        item_sums(grad_head_scale, share_hits),
        item_sums(head_in_grad, share_hits),
    )
    items = jnp.concatenate(local_items, axis=-1).reshape(-1, D)
    items = jnp.sum(gather_small(items, ("mp",), 5), 0).astype(BF)
    mod_grad = gather_small(items, ("dp",), 6).reshape(count_dp * rows * ITEMS, 8 * D)
    cond_part = jnp.where(owns_ada, contract_last(mod_grad, w_ada), 0.0)
    cond_grad = silu_back(jnp.sum(gather_small(cond_part, ("dp",), 7), 0))[0]

    def gram(values):
        return lax.dot_general(
            values, values, (((1,), (1,)), ((), ())), precision=HIGH, preferred_element_type=F32
        )

    same_class = (all_labels[:, None] == all_labels[None, :]).astype(F32)
    squares = (
        jnp.sum(share_head * share_head)
        + jnp.sum(share_down * share_down)
        + jnp.sum(share_up * share_up)
        + jnp.sum(share_attn * share_attn)
        + jnp.where(
            owns_ada, jnp.sum(gram(cond_act.astype(F32)) * gram(mod_grad.astype(F32))), 0.0
        )
        + jnp.where(owns_class, jnp.sum(same_class * gram(cond_grad)), 0.0)
    )
    terms = jnp.stack((squares, loss_term) + square_terms)
    terms = jnp.pad(terms.reshape(1, -1), ((0, 7), (0, LANES - terms.shape[0])))
    norm_terms = jnp.sum(gather_small(terms, ("dp", "mp"), 8)[:, 0, :], 0)
    grad_norm = jnp.sqrt(norm_terms[0])
    loss = norm_terms[1] / count
    factor = jnp.minimum(1.0, CLIP_AT / (grad_norm + 1e-06))

    chunk = jnp.zeros((count_dp, k_slot, block, D), BF)
    summed_shares = [
        share_attn[:k_qkv],
        share_attn[k_qkv:],
        share_up,
        share_down,
        share_head,
    ]
    for m, part in zip(matrix_of, summed_shares):
        chunk = lax.dynamic_update_slice(chunk, part.astype(BF)[None], (owners[m], 0, 0, 0))
    got = lax.all_to_all(chunk, "dp", 0, 0, tiled=True)
    slot_grad = got.transpose(1, 0, 2, 3).reshape(slot_rows, D)
    class_parts = jnp.concatenate(
        [jnp.where((all_labels % ways == part)[:, None], cond_grad, 0.0) for part in range(ways)],
        -1,
    )
    class_grad = lax.dot_general(
        (all_labels[:, None] // ways == row_ids[None, :]).astype(F32),
        class_parts,
        (((0,), (0,)), ((), ())),
        precision=HIGH,
        preferred_element_type=F32,
    )
    slot_fill = jnp.zeros((), jnp.int32)
    for m, size in zip(matrix_of + [6], row_counts + [CLASSES // ways]):
        slot_fill = jnp.where(owners[m] == mine, size, slot_fill)
    ada_fill = jnp.where(owns_ada, 3 * slot, 0)

    count_step = step[0].astype(F32)
    fix_one = 1.0 - BETA_ONE**count_step
    fix_two = 1.0 - BETA_TWO**count_step

    outs = adam_step(
        jnp.stack([factor, fix_one, fix_two]),
        jnp.stack([slot_fill, owns_class.astype(jnp.int32), ada_fill]),
        slot_grad,
        class_grad,
        cond_act.T,
        mod_grad,
        master_view,
        first_view,
        second_view,
    )
    outs = [value.reshape(master.shape) for value in outs]
    act_rms = jnp.sqrt(norm_terms[2:5] / (count * D))
    return (loss, grad_norm, act_rms, *outs)


def solution(mesh):
    placed = (
        P("dp", None, None),
        P("dp", None),
        P("dp", None),
        P("dp", None),
        P("dp", None),
        P("dp", None),
        P(),
        P(),
        P("dp", "mp", None),
        P("dp", "mp", None),
        P("dp", "mp", None),
    )
    return jax.shard_map(
        per_device,
        mesh=mesh,
        in_specs=placed,
        out_specs=(P(), P(), P(), P("dp", "mp", None), P("dp", "mp", None), P("dp", "mp", None)),
        check_vma=False,
    )
```
